32 devices in a mesh: batch: 4 (over z), seq: 8 (over y, x, core).
Axes of the slice: x: 2, y: 2, z: 4, core: 2. Of those that a mesh axis runs over, the one named last changes fastest.
Arguments:
- tokens: bfloat16 [2, 64, 8192], P(None, 'batch', 'seq'), may hold values from -8 to 8
- norm_gain: bfloat16 [8192], P('seq'), may hold values from 0.5 to 1.5
- w_qkv: bfloat16 [8192, 10240], P('batch', 'seq'), may hold values from -0.0625 to 0.0625
- w_out: bfloat16 [8192, 8192], P('seq'), may hold values from -0.75 to 0.75
- cache_keys: bfloat16 [64, 1024, 1024], P('batch', 'seq'), may hold values from -120 to 120
- cache_values: bfloat16 [64, 1024, 1024], P('batch', 'seq'), may hold values from -6 to 6
- lengths: int32 [64], P('batch'), may hold values from 256 to 1022
- positions: int32 [64], P('batch'), may hold values from 0 to 4095
Outputs:
- mixed: bfloat16 [2, 64, 8192], P(None, 'batch', 'seq')
The draws below stay inside these ranges and needn't reach their ends.
Inputs may be any that keep to these rules, and one draw needn't show every extreme that they name: `lengths`: filled cache positions of a sequence; its two new tokens take the next two positions.
All inputs are finite; a program needn't handle non-finite values.
Results may differ from the reference program's by a relative error of at most 0.01255.
The reference program's roundings to bfloat16 on the way (of `normed`, `projected`, `rounded` and `attended`) count: a program that leaves them out, or rounds other values in their place, can miss the bound.
Values may be sent and summed in bfloat16 or wider, within the bound.
A program may use at most 128 MiB of HBM per device.

```python
import math
import jax
import jax.numpy as jnp
from jax import lax

D = 8192
H = 64
KVH = 8
HD = 128
CTX_DEV = 128
SEQS = 64
CTX = 1024
KVW = 1024
QKV = 10240
N_SEQ = 8


def draw_tokens(key, part):
    first, second, third = jax.random.split(jax.random.fold_in(key, 11), 3)
    shape = (2, SEQS, D)
    rising = jnp.exp(jnp.linspace(0.0, math.log(3.0), D)).astype(jnp.float32)
    jitter = jax.random.uniform(third, (1, 1, D), jnp.float32, 0.5, 1.5)
    base = jax.random.normal(first, shape, jnp.float32)
    scales = jnp.exp(jax.random.uniform(second, (2, SEQS, 1), jnp.float32, math.log(0.15), math.log(1.5)))
    return jnp.clip(base * scales * rising * jitter * 0.8, -8.0, 8.0).astype(jnp.bfloat16)


def draw_cache_keys(key, part):
    source = jax.random.fold_in(key, 23)
    base = jax.random.normal(source, (SEQS, CTX, KVW), jnp.float32)
    return jnp.clip(base * 2.0, -12.0, 12.0).astype(jnp.bfloat16)


def set_ends(array, key, low, largest):
    dims = array.shape
    index_at = [jax.random.randint(jax.random.fold_in(key, axis), (), 0, dims[axis]) for axis in range(len(dims))]
    array = array.at[tuple(index_at)].set(low)
    longest = dims.index(max(dims))
    index_at[longest] = (index_at[longest] + 1) % dims[longest]
    return array.at[tuple(index_at)].set(largest)


def strengthened(entries, rng, source, target, shards_of, factor):
    def block_of(position):
        return (jnp.arange(entries.shape[position]) // (entries.shape[position] // shards_of)).reshape((-1,) + (1,) * (entries.ndim - 1 - position))

    one_side = jax.random.permutation(rng, shards_of)[block_of(target)]
    far = (block_of(target) + shards_of // 2) % shards_of
    return jnp.where((block_of(source) == one_side) | (block_of(source) == far), factor * entries, entries)


def levels(rng, dims, shards, low, high):
    def one(position, parts):
        steps = jax.random.uniform(jax.random.fold_in(jax.random.fold_in(rng, 6), position), (parts,), jnp.float32, low / len(shards), high / len(shards))
        return jnp.repeat(jnp.exp(steps), dims[position] // parts).reshape((-1,) + (1,) * (len(dims) - position - 1))

    factor_of = one(*shards[0])
    for cut in shards[1:]:
        factor_of = factor_of * one(*cut)
    return factor_of


def centred(key, shape, scale, limit, cuts=(), kind=jnp.bfloat16):
    result = scale * jax.random.normal(key, shape, jnp.float32)
    if cuts:
        result = result * levels(key, shape, cuts, -0.22, 0.18)
    return jnp.clip(result, -limit, limit).astype(kind)


def heavy_noise(own_key, extent, spread, bound, shards, heavy, dtype=jnp.bfloat16):
    result = spread * jax.random.normal(own_key, extent, jnp.float32)
    if shards:
        result = result * levels(own_key, extent, shards, -0.22, 0.18)
    return jnp.clip(strengthened(result, jax.random.fold_in(own_key, 3), *heavy), -bound, bound).astype(dtype)


def setup_inputs(seed: int = 0) -> dict:
    arg_keys = jax.random.split(jax.random.key(seed), 9)
    return {
        "tokens": draw_tokens(jax.random.fold_in(arg_keys[8], 71), 0),
        "norm_gain": jnp.clip(1.0 + 0.1 * jax.random.normal(arg_keys[1], (D,), jnp.float32), 0.5, 1.5).astype(jnp.bfloat16),
        "w_qkv": centred(arg_keys[2], (D, QKV), D ** -0.5, 0.0625, ((0, 4), (1, 8))),
        "w_out": heavy_noise(arg_keys[3], (H * HD, D), HD ** -0.5, 0.75, ((0, 8),), (0, 1, 8, 2.0)),
        "cache_keys": draw_cache_keys(jax.random.fold_in(arg_keys[8], 71), 0),
        "cache_values": centred(arg_keys[5], (SEQS, CTX, KVW), 1.0, 6.0, ((0, 4), (1, 8))),
        "lengths": set_ends(jax.random.randint(arg_keys[6], (SEQS,), CTX // 4, CTX - 1), jax.random.fold_in(arg_keys[6], 1), CTX // 4, (CTX - 1) - 1).astype(jnp.int32),
        "positions": set_ends(jax.random.randint(arg_keys[7], (SEQS,), 0, 4 * CTX), jax.random.fold_in(arg_keys[7], 1), 0, (4 * CTX) - 1).astype(jnp.int32),
    }


rope_base = 500000.0
epsilon = 1e-05
lowest = -1e+30

def rotate(heads, places):
    half = heads.shape[-1] // 2
    freqs = rope_base ** (-(jnp.arange(half).astype(jnp.float32) * 2.0) / heads.shape[-1])
    angles = places[:, None, None] * freqs
    cosine = jnp.cos(angles)
    sine = jnp.sin(angles)
    first = heads[..., :half]
    second = heads[..., half:]
    return jnp.concatenate([first * cosine - second * sine, second * cosine + first * sine], -1)

def normalize(rows, gain):
    widened = rows.astype(jnp.float32)
    totals = lax.optimization_barrier(jnp.sum(widened * widened, -1, keepdims=True))
    return (widened * lax.rsqrt(totals / rows.shape[-1] + epsilon) * gain.astype(jnp.float32)).astype(jnp.bfloat16)

def reference(tokens, norm_gain, w_qkv, w_out, cache_keys, cache_values, lengths, positions):
    seqs = tokens.shape[1]
    width = tokens.shape[2]
    group = H // KVH
    query_width = H * HD
    pair_width = KVH * HD
    flat = tokens.reshape(2 * seqs, width)
    normed = normalize(flat, norm_gain)
    projected = jnp.dot(normed, w_qkv, preferred_element_type=jnp.float32).astype(jnp.bfloat16)
    places = jnp.concatenate([positions, positions + 1]).astype(jnp.float32)
    queries = rotate(projected[:, :query_width].astype(jnp.float32).reshape(2 * seqs, H, HD), places).astype(jnp.bfloat16)
    fresh_keys = rotate(projected[:, query_width:query_width + pair_width].astype(jnp.float32).reshape(2 * seqs, KVH, HD), places).astype(jnp.bfloat16)
    fresh_values = projected[:, query_width + pair_width:].reshape(2 * seqs, KVH, HD)
    queries = jnp.transpose(queries.reshape(2, seqs, H, HD), (1, 0, 2, 3))
    fresh_keys = jnp.transpose(fresh_keys.reshape(2, seqs, KVH, HD), (1, 0, 2, 3))
    fresh_values = jnp.transpose(fresh_values.reshape(2, seqs, KVH, HD), (1, 0, 2, 3))

    def attend(items):
        query_pair, key_pair, value_pair, keys, values, length = items
        block_keys = keys.reshape(N_SEQ, CTX_DEV, KVH, HD).astype(jnp.float32)
        block_values = values.reshape(N_SEQ, CTX_DEV, KVH, HD).astype(jnp.float32)
        grouped = query_pair.astype(jnp.float32).reshape(2, KVH, group, HD)
        scores = jnp.einsum('tkgd,snkd->tkgsn', grouped, block_keys) / math.sqrt(HD)
        extra = jnp.einsum('tkgd,jkd->tkgj', grouped, key_pair.astype(jnp.float32)) / math.sqrt(HD)
        extra = extra[:, :, :, None, :]
        place = jnp.arange(N_SEQ).astype(jnp.int32)[:, None] * CTX_DEV + jnp.arange(CTX_DEV).astype(jnp.int32)[None, :]
        live_cache = (place < length)[None, None, None, :, :]
        pair_index = jnp.arange(2).astype(jnp.int32)
        owner = (length + pair_index)[None, :] // CTX_DEV == jnp.arange(N_SEQ).astype(jnp.int32)[:, None]
        causal = pair_index[None, :] <= pair_index[:, None]
        live_extra = (owner[None, :, :] & causal[:, None, :])[:, None, None, :, :]
        block_peak = jnp.maximum(lax.optimization_barrier(jnp.max(jnp.where(live_cache, scores, lowest), -1)), lax.optimization_barrier(jnp.max(jnp.where(live_extra, extra, lowest), -1)))
        weights = jnp.where(live_cache, jnp.exp(scores - block_peak[..., None]), 0.0)
        extra_weights = jnp.where(live_extra, jnp.exp(extra - block_peak[..., None]), 0.0)
        block_total = lax.optimization_barrier(jnp.sum(weights, -1)) + lax.optimization_barrier(jnp.sum(extra_weights, -1))
        rounded = lax.optimization_barrier(weights.astype(jnp.bfloat16)).astype(jnp.float32)
        extra_rounded = lax.optimization_barrier(extra_weights.astype(jnp.bfloat16)).astype(jnp.float32)
        block_sum = jnp.einsum('tkgsn,snkd->tkgsd', rounded, block_values)
        block_sum = block_sum + jnp.einsum('tkgsj,jkd->tkgsd', extra_rounded, value_pair.astype(jnp.float32))
        peak = lax.optimization_barrier(jnp.max(block_peak, -1, keepdims=True))
        factor = jnp.exp(block_peak - peak)
        summed = lax.optimization_barrier(jnp.sum(factor[..., None] * block_sum, 3))
        total = lax.optimization_barrier(jnp.sum(factor * block_total, 3))
        return (summed / total[..., None]).astype(jnp.bfloat16).reshape(2, H * HD)
    attended = lax.map(attend, (queries, fresh_keys, fresh_values, cache_keys, cache_values, lengths))
    attended = jnp.transpose(attended, (1, 0, 2)).reshape(2 * seqs, H * HD)
    output = jnp.dot(attended, w_out, preferred_element_type=jnp.float32)
    return (flat.astype(jnp.float32) + output).astype(jnp.bfloat16).reshape(2, seqs, width)
```

```python
import math

import jax
import jax.numpy as jnp
from jax import lax
from jax.experimental import pallas as pl
from jax.experimental.pallas import tpu as pltpu
from jax.sharding import PartitionSpec as P

D = 8192
H = 64
KVH = 8
HD = 128
LANES = 128
PAD = 16
MESH = pl.DeviceIdType.MESH

rope_base = 500000.0
epsilon = 1e-05
lowest = -1e30


def flip(index, bits):
    result = index
    step = 1
    while step <= bits:
        if bits & step:
            result = result + step * (1 - 2 * ((index // step) % 2))
        step *= 2
    return result


def remote(src, dst, send_sem, recv_sem, batch, seq):
    return pltpu.make_async_remote_copy(
        src_ref=src,
        dst_ref=dst,
        send_sem=send_sem,
        recv_sem=recv_sem,
        device_id=(batch, seq),
        device_id_type=MESH,
    )


def signal(sem, batch, seq):
    pl.semaphore_signal(sem, inc=1, device_id=(batch, seq), device_id_type=MESH)


def project_kernel(
    nbatch, nseq, x_ref, gain_ref, w_hbm, out_ref,
    wbuf, stat_send, stat_recv, normed, slots, part, part_recv, gath,
    w_sem, s1, r1, s2, r2, s3, r3, s4, r4,
):
    b = lax.axis_index("batch")
    s = lax.axis_index("seq")
    sub = nseq // nbatch
    rows, local = x_ref.shape
    width = wbuf.shape[1]
    w_copy = pltpu.make_async_copy(w_hbm, wbuf, w_sem)
    w_copy.start()

    home = s // sub
    place = s % sub
    at_home = home == b
    barrier = pltpu.get_barrier_semaphore()
    for k in range(1, nseq):
        signal(barrier, b, flip(s, k))
    for k in range(1, nbatch):
        signal(barrier, flip(b, k), s)
    for source in range(nbatch):
        for j in range(sub):
            @pl.when(jnp.logical_not((source == b) & (b * sub + j == s)))
            def _():
                signal(barrier, source, b * sub + j)

    widened = x_ref[...].astype(jnp.float32)
    sums = jnp.sum(widened * widened, -1, keepdims=True)
    tiles = rows // 8
    span = LANES // tiles
    lane = lax.broadcasted_iota(jnp.int32, (8, LANES), 1) // span
    packed = jnp.zeros((8, LANES), jnp.float32)
    for i in range(tiles):
        packed = jnp.where(lane == i, sums[i * 8 : (i + 1) * 8], packed)
    stat_send[...] = packed

    pl.semaphore_wait(barrier, (nseq - 1) + (nbatch - 1) + nseq - jnp.where(at_home, 1, 0))

    copies = []
    for k in range(nseq - 1, 0, -1):
        copies.append(remote(stat_send, stat_recv.at[k], s1.at[k], r1.at[k], b, flip(s, k)))
        copies[-1].start()
    total = packed
    for copy in copies:
        copy.wait_recv()
    for k in range(1, nseq):
        total = total + stat_recv[k]
    gain = gain_ref[...].astype(jnp.float32)
    inverse = lax.rsqrt(total / D + epsilon)
    column = jnp.concatenate([inverse[:, i * span : i * span + 1] for i in range(tiles)], 0)
    normed[...] = (widened * column * gain).astype(jnp.bfloat16)

    mine = pl.ds(pl.multiple_of(b * rows, rows), rows)
    sends = []
    for k in range(nseq - 1, 0, -1):
        sends.append(
            remote(normed, slots.at[place, mine], s2.at[k], r2.at[b, place], home, flip(s, k))
        )
        sends[-1].start()
    straight = remote(normed, slots.at[place, mine], s2.at[0], r2.at[b, place], home, s)

    @pl.when(jnp.logical_not(at_home))
    def _():
        straight.start()

    @pl.when(at_home)
    def _():
        slots[place, mine, :] = normed[...]

    for source in range(nbatch):
        for j in range(sub):
            @pl.when(jnp.logical_not((source == b) & (b * sub + j == s)))
            def _():
                remote(
                    normed, slots.at[j, pl.ds(source * rows, rows)],
                    s2.at[0], r2.at[source, j], source, b * sub + j,
                ).wait_recv()

    w_copy.wait()
    chunk = 256 if width % 256 == 0 else width
    for c in range(0, width, chunk):
        acc = None
        for j in range(sub):
            term = jnp.dot(
                slots[j], wbuf[j * local : (j + 1) * local, c : c + chunk],
                preferred_element_type=jnp.float32,
            )
            acc = term if acc is None else acc + term
        part[:, c : c + chunk] = acc

    reduces = []
    for k in range(nbatch - 1, 0, -1):
        to = flip(b, k)
        reduces.append(
            remote(
                part.at[pl.ds(pl.multiple_of(to * rows, rows), rows)],
                part_recv.at[k], s3.at[k], r3.at[k], to, s,
            )
        )
        reduces[-1].start()
    for copy in reduces:
        copy.wait_recv()
    owned = part[mine, :]
    for k in range(1, nbatch):
        owned = owned + part_recv[k]
    gath[s] = owned.astype(jnp.bfloat16)

    gathers = []
    for k in range(nseq - 1, 0, -1):
        gathers.append(remote(gath.at[s], gath.at[s], s4.at[k], r4.at[s], b, flip(s, k)))
        gathers[-1].start()
    for source in range(nseq):
        @pl.when(source != s)
        def _():
            remote(gath.at[source], gath.at[source], s4.at[0], r4.at[source], b, source).wait_recv()

        if len(out_ref.shape) == 2:
            out_ref[:, source * width : (source + 1) * width] = gath[source]
        else:
            out_ref[source] = gath[source]

    for copy in copies + sends + reduces + gathers:
        copy.wait_send()

    @pl.when(jnp.logical_not(at_home))
    def _():
        straight.wait_send()


def attend_kernel(
    nseq, length_ref, x_ref, q_ref, fresh_k, fresh_v, keys_hbm, values_hbm, w_hbm, out_ref,
    kext, vext, wbuf, wide_q, stat, o_send, o_recv, st_send, st_recv, heads, attended,
    p_send, p_recv,
    k_sem, v_sem, fk_sem, fv_sem, w_sem, s1, r1, s2, r2, s3, r3,
):
    b = lax.axis_index("batch")
    s = lax.axis_index("seq")
    seqs, shard_len, _ = keys_hbm.shape
    rows, local = x_ref.shape
    here = H // nseq
    pair_rows = 2 * (H // KVH)
    per = 2 * here
    split = pair_rows // per
    depth = shard_len + PAD
    scale = 1.0 / math.sqrt(HD)

    loads = []
    fresh_copies = [
        pltpu.make_async_copy(fresh_k, kext.at[:, pl.ds(shard_len, PAD)], fk_sem),
        pltpu.make_async_copy(fresh_v, vext.at[:, pl.ds(shard_len, PAD)], fv_sem),
    ]
    key_copies = [
        pltpu.make_async_copy(keys_hbm.at[i], kext.at[i, pl.ds(0, shard_len)], k_sem.at[i])
        for i in range(seqs)
    ]
    value_copies = [
        pltpu.make_async_copy(values_hbm.at[i], vext.at[i, pl.ds(0, shard_len)], v_sem.at[i])
        for i in range(seqs)
    ]
    order = list(range(nseq - 1, -1, -1))
    weight_copies = {}
    for k in order:
        to = flip(s, k)
        weight_copies[k] = pltpu.make_async_copy(
            w_hbm.at[:, pl.ds(pl.multiple_of(to * local, local), local)], wbuf.at[k], w_sem.at[k]
        )
    for copy in fresh_copies + key_copies + value_copies + [weight_copies[k] for k in order]:
        copy.start()

    barrier = pltpu.get_barrier_semaphore()
    for k in range(1, nseq):
        signal(barrier, b, flip(s, k))

    wide_q[...] = jnp.zeros_like(wide_q)
    stat[...] = jnp.zeros_like(stat)
    for i in range(seqs):
        for k in range(KVH):
            wide_q[i, k * pair_rows : (k + 1) * pair_rows, k * HD : (k + 1) * HD] = q_ref[
                i, k * pair_rows : (k + 1) * pair_rows
            ]
    for copy in fresh_copies:
        copy.wait()

    columns = KVH * pair_rows
    row = lax.broadcasted_iota(jnp.int32, (depth, columns), 0)
    lane = lax.broadcasted_iota(jnp.int32, (depth, columns), 1)
    step = (lane // here) % 2
    low = s * shard_len
    cached = row < shard_len
    causal = (row >= shard_len) & (row - shard_len <= step)
    for i in range(seqs):
        key_copies[i].wait()
        value_copies[i].wait()
        scores = lax.dot_general(
            kext[i], wide_q[i], (((1,), (1,)), ((), ())), preferred_element_type=jnp.float32
        ) * scale
        length = jnp.full((depth, columns), length_ref[i], jnp.int32)
        fresh_place = length + row - shard_len
        live = (cached & (low + row < length)) | (
            causal & (fresh_place >= low) & (fresh_place < low + shard_len)
        )
        peak = jnp.max(jnp.where(live, scores, lowest), 0, keepdims=True)
        weights = jnp.where(live, jnp.exp(scores - peak), 0.0)
        stat[i : i + 1, :] = peak
        stat[64 + i : 65 + i, :] = jnp.sum(weights, 0, keepdims=True)
        block = lax.dot_general(
            weights.astype(jnp.bfloat16), vext[i], (((0,), (0,)), ((), ())),
            preferred_element_type=jnp.float32,
        )
        for k in range(KVH):
            for g in range(split):
                first = k * pair_rows + g * per
                o_send[k * split + g, i] = block[first : first + per, k * HD : (k + 1) * HD].astype(
                    jnp.bfloat16
                )
    turned = jnp.transpose(stat[...])
    for k in range(nseq):
        st_send[k] = turned[k * per : (k + 1) * per]

    pl.semaphore_wait(barrier, nseq - 1)
    sends = []
    for k in range(nseq - 1, 0, -1):
        to = flip(s, k)
        sends.append(remote(st_send.at[to], st_recv.at[k], s1.at[k], r1.at[k], b, to))
        sends[-1].start()
        sends.append(remote(o_send.at[to], o_recv.at[k], s2.at[k], r2.at[k], b, to))
        sends[-1].start()
    st_recv[0] = st_send[s]
    o_recv[0] = o_send[s]
    for copy in sends:
        copy.wait_recv()

    stats = [st_recv[k] for k in range(nseq)]
    peak = stats[0]
    for k in range(1, nseq):
        peak = jnp.maximum(peak, stats[k])
    factors = [jnp.exp(stats[k] - peak) for k in range(nseq)]
    total = None
    for k in range(nseq):
        term = pltpu.roll(factors[k], 64, 1) * stats[k]
        total = term if total is None else total + term
    for i in range(seqs):
        acc = None
        for k in range(nseq):
            term = factors[k][:, i : i + 1] * o_recv[k, i].astype(jnp.float32)
            acc = term if acc is None else acc + term
        heads[i] = acc / total[:, 64 + i : 65 + i]
    for t in range(2):
        for g in range(here):
            attended[t * seqs : (t + 1) * seqs, g * HD : (g + 1) * HD] = heads[
                :, t * here + g, :
            ].astype(jnp.bfloat16)

    result = x_ref[...].astype(jnp.float32)
    outs = []
    for k in order:
        weight_copies[k].wait()
        value = jnp.dot(attended[...], wbuf[k], preferred_element_type=jnp.float32)
        if k:
            p_send[k] = value.astype(jnp.bfloat16)
            outs.append(remote(p_send.at[k], p_recv.at[k], s3.at[k], r3.at[k], b, flip(s, k)))
            outs[-1].start()
        else:
            own = value
    for copy in outs:
        copy.wait_recv()
    for k in range(1, nseq):
        own = own + p_recv[k].astype(jnp.float32)
    out_ref[...] = (result + own).astype(jnp.bfloat16)
    for copy in sends + outs:
        copy.wait_send()


def rotate(heads, places):
    half = heads.shape[-1] // 2
    freqs = rope_base ** (-(jnp.arange(half).astype(jnp.float32) * 2.0) / heads.shape[-1])
    angles = places[:, None, None] * freqs
    cosine = jnp.cos(angles)
    sine = jnp.sin(angles)
    first = heads[..., :half]
    second = heads[..., half:]
    return jnp.concatenate([first * cosine - second * sine, second * cosine + first * sine], -1)


def shards(tokens, norm_gain, w_qkv, w_out, cache_keys, cache_values, lengths, positions):
    nbatch = lax.axis_size("batch")
    nseq = lax.axis_size("seq")
    seqs = tokens.shape[1]
    local = tokens.shape[2]
    rows = 2 * seqs
    width = w_qkv.shape[1]
    sub = nseq // nbatch
    group = H // KVH
    here = H // nseq
    split = group // here
    query_width = H * HD
    pair_width = KVH * HD
    shard_len = cache_keys.shape[1]
    flat = tokens.reshape(rows, local)
    vmem = pl.BlockSpec(memory_space=pltpu.VMEM)
    hbm = pl.BlockSpec(memory_space=pl.ANY)
    dma = pltpu.SemaphoreType.DMA
    f32 = jnp.float32
    bf16 = jnp.bfloat16

    joined = width % LANES == 0
    projected = pl.pallas_call(
        lambda *refs: project_kernel(nbatch, nseq, *refs),
        name="project",
        out_shape=jax.ShapeDtypeStruct(
            (rows, nseq * width) if joined else (nseq, rows, width), bf16
        ),
        in_specs=[vmem, vmem, hbm],
        out_specs=vmem,
        scratch_shapes=[
            pltpu.VMEM(w_qkv.shape, bf16),
            pltpu.VMEM((8, LANES), f32),
            pltpu.VMEM((nseq, 8, LANES), f32),
            pltpu.VMEM((rows, local), bf16),
            pltpu.VMEM((sub, nbatch * rows, local), bf16),
            pltpu.VMEM((nbatch * rows, width), f32),
            pltpu.VMEM((nbatch, rows, width), f32),
            pltpu.VMEM((nseq, rows, width), bf16),
            dma,
            dma((nseq,)), dma((nseq,)),
            dma((nseq,)), dma((nbatch, sub)),
            dma((nbatch,)), dma((nbatch,)),
            dma((nseq,)), dma((nseq,)),
        ],
        compiler_params=pltpu.CompilerParams(
            collective_id=0, has_side_effects=True, vmem_limit_bytes=40 * 1024 * 1024
        ),
    )(flat, norm_gain.reshape(1, local), w_qkv)
    if not joined:
        projected = jnp.transpose(projected, (1, 0, 2)).reshape(rows, nseq * width)

    places = jnp.concatenate([positions, positions + 1]).astype(f32)
    queries = rotate(
        projected[:, :query_width].astype(f32).reshape(rows, H, HD), places
    ).astype(bf16)
    fresh_keys = rotate(
        projected[:, query_width : query_width + pair_width].astype(f32).reshape(rows, KVH, HD),
        places,
    ).astype(bf16)
    fresh_values = projected[:, query_width + pair_width :]
    queries = jnp.transpose(
        queries.reshape(2, seqs, KVH, split, here, HD), (1, 2, 3, 0, 4, 5)
    ).reshape(seqs, 2 * H, HD)

    def padded(fresh):
        fresh = jnp.transpose(fresh.reshape(2, seqs, pair_width), (1, 0, 2))
        return jnp.pad(fresh, ((0, 0), (0, PAD - 2), (0, 0)))

    depth = shard_len + PAD
    per = 2 * here
    smem = pl.BlockSpec(memory_space=pltpu.SMEM)
    mixed = pl.pallas_call(
        lambda *refs: attend_kernel(nseq, *refs),
        name="attend",
        out_shape=jax.ShapeDtypeStruct((rows, local), bf16),
        in_specs=[smem, vmem, vmem, hbm, hbm, hbm, hbm, hbm],
        out_specs=vmem,
        scratch_shapes=[
            pltpu.VMEM((seqs, depth, pair_width), bf16),
            pltpu.VMEM((seqs, depth, pair_width), bf16),
            pltpu.VMEM((nseq, w_out.shape[0], local), bf16),
            pltpu.VMEM((seqs, 2 * H, pair_width), bf16),
            pltpu.VMEM((LANES, 2 * H), f32),
            pltpu.VMEM((nseq, seqs, per, HD), bf16),
            pltpu.VMEM((nseq, seqs, per, HD), bf16),
            pltpu.VMEM((nseq, per, LANES), f32),
            pltpu.VMEM((nseq, per, LANES), f32),
            pltpu.VMEM((seqs, per, HD), f32),
            pltpu.VMEM((rows, here * HD), bf16),
            pltpu.VMEM((nseq, rows, local), bf16),
            pltpu.VMEM((nseq, rows, local), bf16),
            dma((seqs,)), dma((seqs,)), dma, dma, dma((nseq,)),
            dma((nseq,)), dma((nseq,)),
            dma((nseq,)), dma((nseq,)),
            dma((nseq,)), dma((nseq,)),
        ],
        compiler_params=pltpu.CompilerParams(
            collective_id=1, has_side_effects=True, vmem_limit_bytes=60 * 1024 * 1024
        ),
    )(lengths, flat, queries, padded(fresh_keys), padded(fresh_values), cache_keys, cache_values, w_out)
    return mixed.reshape(2, seqs, local)


def solution(mesh):
    return jax.shard_map(
        shards,
        mesh=mesh,
        in_specs=(
            P(None, "batch", "seq"),
            P("seq"),
            P("batch", "seq"),
            P("seq", None),
            P("batch", "seq", None),
            P("batch", "seq", None),
            P("batch"),
            P("batch"),
        ),
        out_specs=P(None, "batch", "seq"),
        check_vma=False,
    )
```

```python
import math

import jax
import jax.numpy as jnp
from jax import lax
from jax.experimental import pallas as pl
from jax.experimental.pallas import tpu as pltpu
from jax.sharding import PartitionSpec as P

D = 8192
H = 64
KVH = 8
HD = 128
LANES = 128
PAD = 16
MESH = pl.DeviceIdType.MESH

rope_base = 500000.0
epsilon = 1e-05
lowest = -1e30


def flip(index, bits):
    result = index
    step = 1
    while step <= bits:
        if bits & step:
            result = result + step * (1 - 2 * ((index // step) % 2))
        step *= 2
    return result


def remote(src, dst, send_sem, recv_sem, batch, seq):
    return pltpu.make_async_remote_copy(
        src_ref=src,
        dst_ref=dst,
        send_sem=send_sem,
        recv_sem=recv_sem,
        device_id=(batch, seq),
        device_id_type=MESH,
    )


def signal(sem, batch, seq):
    pl.semaphore_signal(sem, inc=1, device_id=(batch, seq), device_id_type=MESH)


def project_kernel(
    nbatch, nseq, x_ref, gain_ref, w_hbm, out_ref,
    wbuf, stat_send, stat_recv, normed, plane, slots, part, part_recv, gath,
    w_sem, s1, r1, s2, r2, s3, r3, s4, r4, s5, r5, s6, r6, s7,
):
    b = lax.axis_index("batch")
    s = lax.axis_index("seq")
    sub = nseq // nbatch
    rows, local = x_ref.shape
    width = wbuf.shape[1]
    w_copy = pltpu.make_async_copy(w_hbm, wbuf, w_sem)
    w_copy.start()

    home = s // sub
    place = s % sub
    barrier = pltpu.get_barrier_semaphore()
    for k in range(1, nseq):
        signal(barrier, b, flip(s, k))
    for k in range(1, nbatch):
        signal(barrier, flip(b, k), s)

    widened = x_ref[...].astype(jnp.float32)
    sums = jnp.sum(widened * widened, -1, keepdims=True)
    tiles = rows // 8
    span = LANES // tiles
    lane = lax.broadcasted_iota(jnp.int32, (8, LANES), 1) // span
    packed = jnp.zeros((8, LANES), jnp.float32)
    for i in range(tiles):
        packed = jnp.where(lane == i, sums[i * 8 : (i + 1) * 8], packed)
    stat_send[...] = packed

    pl.semaphore_wait(barrier, (nseq - 1) + (nbatch - 1))

    copies = []
    for k in range(nseq - 1, 0, -1):
        copies.append(remote(stat_send, stat_recv.at[k], s1.at[k], r1.at[k], b, flip(s, k)))
        copies[-1].start()
    total = packed
    for copy in copies:
        copy.wait_recv()
    for k in range(1, nseq):
        total = total + stat_recv[k]
    gain = gain_ref[...].astype(jnp.float32)
    inverse = lax.rsqrt(total / D + epsilon)
    column = jnp.concatenate([inverse[:, i * span : i * span + 1] for i in range(tiles)], 0)
    normed[...] = (widened * column * gain).astype(jnp.bfloat16)

    def strip(batch):
        return pl.ds(pl.multiple_of(batch * rows, rows), rows)

    mine = strip(b)
    sends = []
    for k in range(nbatch - 1, 0, -1):
        peer = flip(home, k) * sub + place
        sends.append(remote(normed, plane.at[k], s2.at[k], r2.at[k], b, peer))
        sends[-1].start()
    onward = []
    for k in range(nbatch):
        target = flip(home, k)
        held = plane.at[k] if k else normed
        copy = remote(held, slots.at[place, mine], s5.at[k], r5.at[b], target, s)
        onward.append((target, copy))
        if k:
            remote(normed, plane.at[k], s2.at[k], r2.at[k], b, target * sub + place).wait_recv()

        @pl.when(target != b)
        def _():
            copy.start()

        @pl.when(target == b)
        def _():
            slots[place, mine, :] = held[...]

    def relay(m, q):
        block = slots.at[place, strip(flip(b, m))]
        to = home * sub + flip(place, q)
        return remote(block, block, s6.at[q, m], r6.at[place, flip(b, m)], b, to)

    for m in range(nbatch):
        other = flip(b, m)
        if m:
            block = slots.at[place, strip(other)]
            remote(block, block, s5.at[0], r5.at[other], other, s).wait_recv()
        for q in range(1, sub):
            sends.append(relay(m, q))
            sends[-1].start()
    for q in range(1, sub):
        for m in range(nbatch):
            other = flip(place, q)
            block = slots.at[other, strip(flip(b, m))]
            remote(
                block, block, s6.at[q, m], r6.at[other, flip(b, m)], b, home * sub + other
            ).wait_recv()

    w_copy.wait()
    chunk = 256 if width % 256 == 0 else width
    for c in range(0, width, chunk):
        acc = None
        for j in range(sub):
            term = jnp.dot(
                slots[j], wbuf[j * local : (j + 1) * local, c : c + chunk],
                preferred_element_type=jnp.float32,
            )
            acc = term if acc is None else acc + term
        part[:, c : c + chunk] = acc

    reduces = []
    for k in range(nbatch - 1, 0, -1):
        to = flip(b, k)
        reduces.append(
            remote(
                part.at[pl.ds(pl.multiple_of(to * rows, rows), rows)],
                part_recv.at[k], s3.at[k], r3.at[k], to, s,
            )
        )
        reduces[-1].start()
    for copy in reduces:
        copy.wait_recv()
    owned = part[mine, :]
    for k in range(1, nbatch):
        owned = owned + part_recv[k]
    gath[s] = owned.astype(jnp.bfloat16)

    gathers = []

    def spread(source, send_sem, to):
        gathers.append(remote(gath.at[source], gath.at[source], send_sem, r4.at[source], b, to))
        gathers[-1].start()

    for k in range(nbatch - 1, 0, -1):
        spread(s, s4.at[k], flip(home, k) * sub + place)
    for k in range(nbatch):
        source = flip(home, k) * sub + place
        if k:
            remote(gath.at[source], gath.at[source], s4.at[k], r4.at[source], b, source).wait_recv()
        for q in range(1, sub):
            spread(source, s7.at[q, k], home * sub + flip(place, q))
    for source in range(nseq):
        @pl.when(source % sub != place)
        def _():
            remote(gath.at[source], gath.at[source], s4.at[0], r4.at[source], b, source).wait_recv()

        if len(out_ref.shape) == 2:
            out_ref[:, source * width : (source + 1) * width] = gath[source]
        else:
            out_ref[source] = gath[source]

    for copy in copies + sends + reduces + gathers:
        copy.wait_send()
    for target, copy in onward:
        @pl.when(target != b)
        def _():
            copy.wait_send()


def attend_kernel(
    nseq, length_ref, x_ref, q_ref, fresh_k, fresh_v, keys_hbm, values_hbm, w_hbm, out_ref,
    kext, vext, wbuf, wide_q, stat, o_send, o_recv, st_send, st_recv, heads, attended,
    p_send, p_recv,
    k_sem, v_sem, fk_sem, fv_sem, w_sem, s1, r1, s2, r2, s3, r3,
):
    b = lax.axis_index("batch")
    s = lax.axis_index("seq")
    seqs, shard_len, _ = keys_hbm.shape
    rows, local = x_ref.shape
    here = H // nseq
    pair_rows = 2 * (H // KVH)
    per = 2 * here
    split = pair_rows // per
    depth = shard_len + PAD
    scale = 1.0 / math.sqrt(HD)

    loads = []
    fresh_copies = [
        pltpu.make_async_copy(fresh_k, kext.at[:, pl.ds(shard_len, PAD)], fk_sem),
        pltpu.make_async_copy(fresh_v, vext.at[:, pl.ds(shard_len, PAD)], fv_sem),
    ]
    key_copies = [
        pltpu.make_async_copy(keys_hbm.at[i], kext.at[i, pl.ds(0, shard_len)], k_sem.at[i])
        for i in range(seqs)
    ]
    value_copies = [
        pltpu.make_async_copy(values_hbm.at[i], vext.at[i, pl.ds(0, shard_len)], v_sem.at[i])
        for i in range(seqs)
    ]
    order = list(range(nseq - 1, -1, -1))
    weight_copies = {}
    for k in order:
        to = flip(s, k)
        weight_copies[k] = pltpu.make_async_copy(
            w_hbm.at[:, pl.ds(pl.multiple_of(to * local, local), local)], wbuf.at[k], w_sem.at[k]
        )
    for copy in fresh_copies + key_copies + value_copies + [weight_copies[k] for k in order]:
        copy.start()

    barrier = pltpu.get_barrier_semaphore()
    for k in range(1, nseq):
        signal(barrier, b, flip(s, k))

    wide_q[...] = jnp.zeros_like(wide_q)
    stat[...] = jnp.zeros_like(stat)
    for i in range(seqs):
        for k in range(KVH):
            wide_q[i, k * pair_rows : (k + 1) * pair_rows, k * HD : (k + 1) * HD] = q_ref[
                i, k * pair_rows : (k + 1) * pair_rows
            ]
    for copy in fresh_copies:
        copy.wait()

    columns = KVH * pair_rows
    row = lax.broadcasted_iota(jnp.int32, (depth, columns), 0)
    lane = lax.broadcasted_iota(jnp.int32, (depth, columns), 1)
    step = (lane // here) % 2
    low = s * shard_len
    cached = row < shard_len
    causal = (row >= shard_len) & (row - shard_len <= step)
    for i in range(seqs):
        key_copies[i].wait()
        value_copies[i].wait()
        scores = lax.dot_general(
            kext[i], wide_q[i], (((1,), (1,)), ((), ())), preferred_element_type=jnp.float32
        ) * scale
        length = jnp.full((depth, columns), length_ref[i], jnp.int32)
        fresh_place = length + row - shard_len
        live = (cached & (low + row < length)) | (
            causal & (fresh_place >= low) & (fresh_place < low + shard_len)
        )
        peak = jnp.max(jnp.where(live, scores, lowest), 0, keepdims=True)
        weights = jnp.where(live, jnp.exp(scores - peak), 0.0)
        stat[i : i + 1, :] = peak
        stat[64 + i : 65 + i, :] = jnp.sum(weights, 0, keepdims=True)
        block = lax.dot_general(
            weights.astype(jnp.bfloat16), vext[i], (((0,), (0,)), ((), ())),
            preferred_element_type=jnp.float32,
        )
        for k in range(KVH):
            for g in range(split):
                first = k * pair_rows + g * per
                o_send[k * split + g, i] = block[first : first + per, k * HD : (k + 1) * HD].astype(
                    jnp.bfloat16
                )
    turned = jnp.transpose(stat[...])
    for k in range(nseq):
        st_send[k] = turned[k * per : (k + 1) * per]

    pl.semaphore_wait(barrier, nseq - 1)
    sends = []
    for k in range(nseq - 1, 0, -1):
        to = flip(s, k)
        sends.append(remote(st_send.at[to], st_recv.at[k], s1.at[k], r1.at[k], b, to))
        sends[-1].start()
        sends.append(remote(o_send.at[to], o_recv.at[k], s2.at[k], r2.at[k], b, to))
        sends[-1].start()
    st_recv[0] = st_send[s]
    o_recv[0] = o_send[s]
    for copy in sends:
        copy.wait_recv()

    stats = [st_recv[k] for k in range(nseq)]
    peak = stats[0]
    for k in range(1, nseq):
        peak = jnp.maximum(peak, stats[k])
    factors = [jnp.exp(stats[k] - peak) for k in range(nseq)]
    total = None
    for k in range(nseq):
        term = pltpu.roll(factors[k], 64, 1) * stats[k]
        total = term if total is None else total + term
    for i in range(seqs):
        acc = None
        for k in range(nseq):
            term = factors[k][:, i : i + 1] * o_recv[k, i].astype(jnp.float32)
            acc = term if acc is None else acc + term
        heads[i] = acc / total[:, 64 + i : 65 + i]
    for t in range(2):
        for g in range(here):
            attended[t * seqs : (t + 1) * seqs, g * HD : (g + 1) * HD] = heads[
                :, t * here + g, :
            ].astype(jnp.bfloat16)

    result = x_ref[...].astype(jnp.float32)
    outs = []
    for k in order:
        weight_copies[k].wait()
        value = jnp.dot(attended[...], wbuf[k], preferred_element_type=jnp.float32)
        if k:
            p_send[k] = value.astype(jnp.bfloat16)
            outs.append(remote(p_send.at[k], p_recv.at[k], s3.at[k], r3.at[k], b, flip(s, k)))
            outs[-1].start()
        else:
            own = value
    for copy in outs:
        copy.wait_recv()
    for k in range(1, nseq):
        own = own + p_recv[k].astype(jnp.float32)
    out_ref[...] = (result + own).astype(jnp.bfloat16)
    for copy in sends + outs:
        copy.wait_send()


def rotate(heads, places):
    half = heads.shape[-1] // 2
    freqs = rope_base ** (-(jnp.arange(half).astype(jnp.float32) * 2.0) / heads.shape[-1])
    angles = places[:, None, None] * freqs
    cosine = jnp.cos(angles)
    sine = jnp.sin(angles)
    first = heads[..., :half]
    second = heads[..., half:]
    return jnp.concatenate([first * cosine - second * sine, second * cosine + first * sine], -1)


def shards(tokens, norm_gain, w_qkv, w_out, cache_keys, cache_values, lengths, positions):
    nbatch = lax.axis_size("batch")
    nseq = lax.axis_size("seq")
    seqs = tokens.shape[1]
    local = tokens.shape[2]
    rows = 2 * seqs
    width = w_qkv.shape[1]
    sub = nseq // nbatch
    group = H // KVH
    here = H // nseq
    split = group // here
    query_width = H * HD
    pair_width = KVH * HD
    shard_len = cache_keys.shape[1]
    flat = tokens.reshape(rows, local)
    vmem = pl.BlockSpec(memory_space=pltpu.VMEM)
    hbm = pl.BlockSpec(memory_space=pl.ANY)
    dma = pltpu.SemaphoreType.DMA
    f32 = jnp.float32
    bf16 = jnp.bfloat16

    joined = width % LANES == 0
    projected = pl.pallas_call(
        lambda *refs: project_kernel(nbatch, nseq, *refs),
        name="project",
        out_shape=jax.ShapeDtypeStruct(
            (rows, nseq * width) if joined else (nseq, rows, width), bf16
        ),
        in_specs=[vmem, vmem, hbm],
        out_specs=vmem,
        scratch_shapes=[
            pltpu.VMEM(w_qkv.shape, bf16),
            pltpu.VMEM((8, LANES), f32),
            pltpu.VMEM((nseq, 8, LANES), f32),
            pltpu.VMEM((rows, local), bf16),
            pltpu.VMEM((nbatch, rows, local), bf16),
            pltpu.VMEM((sub, nbatch * rows, local), bf16),
            pltpu.VMEM((nbatch * rows, width), f32),
            pltpu.VMEM((nbatch, rows, width), f32),
            pltpu.VMEM((nseq, rows, width), bf16),
            dma,
            dma((nseq,)), dma((nseq,)),
            dma((nbatch,)), dma((nbatch,)),
            dma((nbatch,)), dma((nbatch,)),
            dma((nbatch,)), dma((nseq,)),
            dma((nbatch,)), dma((nbatch,)),
            dma((sub, nbatch)), dma((sub, nbatch)),
            dma((sub, nbatch)),
        ],
        compiler_params=pltpu.CompilerParams(
            collective_id=0, has_side_effects=True, vmem_limit_bytes=60 * 1024 * 1024
        ),
    )(flat, norm_gain.reshape(1, local), w_qkv)
    if not joined:
        projected = jnp.transpose(projected, (1, 0, 2)).reshape(rows, nseq * width)

    places = jnp.concatenate([positions, positions + 1]).astype(f32)
    queries = rotate(
        projected[:, :query_width].astype(f32).reshape(rows, H, HD), places
    ).astype(bf16)
    fresh_keys = rotate(
        projected[:, query_width : query_width + pair_width].astype(f32).reshape(rows, KVH, HD),
        places,
    ).astype(bf16)
    fresh_values = projected[:, query_width + pair_width :]
    queries = jnp.transpose(
        queries.reshape(2, seqs, KVH, split, here, HD), (1, 2, 3, 0, 4, 5)
    ).reshape(seqs, 2 * H, HD)

    def padded(fresh):
        fresh = jnp.transpose(fresh.reshape(2, seqs, pair_width), (1, 0, 2))
        return jnp.pad(fresh, ((0, 0), (0, PAD - 2), (0, 0)))

    depth = shard_len + PAD
    per = 2 * here
    smem = pl.BlockSpec(memory_space=pltpu.SMEM)
    mixed = pl.pallas_call(
        lambda *refs: attend_kernel(nseq, *refs),
        name="attend",
        out_shape=jax.ShapeDtypeStruct((rows, local), bf16),
        in_specs=[smem, vmem, vmem, hbm, hbm, hbm, hbm, hbm],
        out_specs=vmem,
        scratch_shapes=[
            pltpu.VMEM((seqs, depth, pair_width), bf16),
            pltpu.VMEM((seqs, depth, pair_width), bf16),
            pltpu.VMEM((nseq, w_out.shape[0], local), bf16),
            pltpu.VMEM((seqs, 2 * H, pair_width), bf16),
            pltpu.VMEM((LANES, 2 * H), f32),
            pltpu.VMEM((nseq, seqs, per, HD), bf16),
            pltpu.VMEM((nseq, seqs, per, HD), bf16),
            pltpu.VMEM((nseq, per, LANES), f32),
            pltpu.VMEM((nseq, per, LANES), f32),
            pltpu.VMEM((seqs, per, HD), f32),
            pltpu.VMEM((rows, here * HD), bf16),
            pltpu.VMEM((nseq, rows, local), bf16),
            pltpu.VMEM((nseq, rows, local), bf16),
            dma((seqs,)), dma((seqs,)), dma, dma, dma((nseq,)),
            dma((nseq,)), dma((nseq,)),
            dma((nseq,)), dma((nseq,)),
            dma((nseq,)), dma((nseq,)),
        ],
        compiler_params=pltpu.CompilerParams(
            collective_id=1, has_side_effects=True, vmem_limit_bytes=60 * 1024 * 1024
        ),
    )(lengths, flat, queries, padded(fresh_keys), padded(fresh_values), cache_keys, cache_values, w_out)
    return mixed.reshape(2, seqs, local)


def solution(mesh):
    return jax.shard_map(
        shards,
        mesh=mesh,
        in_specs=(
            P(None, "batch", "seq"),
            P("seq"),
            P("batch", "seq"),
            P("seq", None),
            P("batch", "seq", None),
            P("batch", "seq", None),
            P("batch"),
            P("batch"),
        ),
        out_specs=P(None, "batch", "seq"),
        check_vma=False,
    )
```
